16 devices in a mesh: fsdp: 16 (over z, y, x, core).
Axes of the slice: x: 2, y: 2, z: 2, core: 2. Of those that a mesh axis runs over, the one named last changes fastest.
Arguments:
- x_in: bfloat16 [16, 384, 1024], P('fsdp')
- positions: int32 [384], replicated
- grad_out: bfloat16 [16, 384, 1024], P('fsdp')
- ln_gamma_1: float32 [1024], P('fsdp')
- w_q_1: bfloat16 [1024, 2048], P('fsdp')
- w_k_1: bfloat16 [1024, 1024], P('fsdp')
- w_v_1: bfloat16 [1024, 1024], P('fsdp')
- w_o_1: bfloat16 [2048, 1024], P('fsdp')
- w_gate_1: bfloat16 [1024, 3072], P('fsdp')
- w_up_1: bfloat16 [1024, 3072], P('fsdp')
- w_down_1: bfloat16 [3072, 1024], P('fsdp')
- q_norm_1: float32 [2048], P('fsdp')
- k_norm_1: float32 [1024], P('fsdp')
- ln_gamma_2: float32 [1024], P('fsdp')
- w_q_2: bfloat16 [1024, 2048], P('fsdp')
- w_k_2: bfloat16 [1024, 1024], P('fsdp')
- w_v_2: bfloat16 [1024, 1024], P('fsdp')
- w_o_2: bfloat16 [2048, 1024], P('fsdp')
- w_gate_2: bfloat16 [1024, 3072], P('fsdp')
- w_up_2: bfloat16 [1024, 3072], P('fsdp')
- w_down_2: bfloat16 [3072, 1024], P('fsdp')
- q_norm_2: float32 [2048], P('fsdp')
- k_norm_2: float32 [1024], P('fsdp')
Outputs:
- output 1: bfloat16 [16, 384, 1024], P('fsdp')
- output 2: bfloat16 [16, 384, 1024], P('fsdp')
- output 3: float32 [1024], P('fsdp')
- output 4: float32 [1024, 2048], P('fsdp')
- output 5: float32 [1024, 1024], P('fsdp')
- output 6: float32 [1024, 1024], P('fsdp')
- output 7: float32 [2048, 1024], P('fsdp')
- output 8: float32 [1024, 3072], P('fsdp')
- output 9: float32 [1024, 3072], P('fsdp')
- output 10: float32 [3072, 1024], P('fsdp')
- output 11: float32 [2048], P('fsdp')
- output 12: float32 [1024], P('fsdp')
- output 13: float32 [1024], P('fsdp')
- output 14: float32 [1024, 2048], P('fsdp')
- output 15: float32 [1024, 1024], P('fsdp')
- output 16: float32 [1024, 1024], P('fsdp')
- output 17: float32 [2048, 1024], P('fsdp')
- output 18: float32 [1024, 3072], P('fsdp')
- output 19: float32 [1024, 3072], P('fsdp')
- output 20: float32 [3072, 1024], P('fsdp')
- output 21: float32 [2048], P('fsdp')
- output 22: float32 [1024], P('fsdp')
All inputs are finite; a program needn't handle non-finite values.
Results may differ from the reference program's by a relative error of at most 0.0197592.
Values are sent between devices in bfloat16 or wider.
A program may use at most 1 GiB of HBM per device.

```python
import functools
import jax
import jax.numpy as jnp
from jax import lax

MODEL_DIM = 1024
NUM_HEADS = 16
KV_HEADS = 8
HEAD_DIM = 128
FFN_DIM = 3072
SEQ_LEN = 384
TOTAL_BATCH = 16

EPSILON = 1e-5
ROPE_THETA = 7.5e7
PARAM_NAMES = ('ln_gamma', 'w_q', 'w_k', 'w_v', 'w_o', 'w_gate', 'w_up', 'w_down', 'q_norm', 'k_norm')


def draw_layer(layer_key):
    sub_keys = jax.random.split(layer_key, 10)
    q_width = NUM_HEADS * HEAD_DIM
    kv_width = KV_HEADS * HEAD_DIM

    def weight(key_w, fan_in, fan_out):
        return (jax.random.normal(key_w, (fan_in, fan_out), jnp.float32) * fan_in ** -0.5).astype(jnp.bfloat16)

    def gain(key_g, width):
        return 1.0 + 0.3 * jax.random.normal(key_g, (width,), jnp.float32)

    return (
        gain(sub_keys[0], MODEL_DIM),
        weight(sub_keys[1], MODEL_DIM, q_width),
        weight(sub_keys[2], MODEL_DIM, kv_width),
        weight(sub_keys[3], MODEL_DIM, kv_width),
        weight(sub_keys[4], q_width, MODEL_DIM),
        weight(sub_keys[5], MODEL_DIM, FFN_DIM),
        weight(sub_keys[6], MODEL_DIM, FFN_DIM),
        weight(sub_keys[7], FFN_DIM, MODEL_DIM),
        gain(sub_keys[8], q_width),
        gain(sub_keys[9], kv_width),
    )


def setup_inputs(seed: int = 0) -> dict:
    root_key = jax.random.key(seed)
    sub_keys = jax.random.split(root_key, 3)
    act_shape = (TOTAL_BATCH, SEQ_LEN, MODEL_DIM)
    pos_gaps = jax.random.randint(sub_keys[1], (SEQ_LEN,), 1, 4, jnp.int32)
    inputs = {
        'x_in': jax.random.normal(sub_keys[0], act_shape, jnp.float32).astype(jnp.bfloat16),
        'positions': (jnp.cumsum(pos_gaps) - pos_gaps[0]).astype(jnp.int32),
        'grad_out': jax.random.normal(sub_keys[2], act_shape, jnp.float32).astype(jnp.bfloat16),
    }
    for layer_index in range(2):
        drawn_params = draw_layer(jax.random.fold_in(root_key, 100 + layer_index))
        for param_name, param_value in zip(PARAM_NAMES, drawn_params):
            inputs[param_name + '_' + str(layer_index + 1)] = param_value
    return inputs


def layer_norm32(values, weight):
    row_mean = jnp.mean(values, axis=-1, keepdims=True)
    centered = values - row_mean
    variance = jnp.mean(centered * centered, axis=-1, keepdims=True)
    return centered * lax.rsqrt(variance + EPSILON) * weight


def rope_tables(positions):
    inv_freq = ROPE_THETA ** (-jnp.arange(0, HEAD_DIM, 2, dtype=jnp.float32) / HEAD_DIM)
    angles = positions.astype(jnp.float32)[:, None] * inv_freq[None, :]
    return jnp.cos(angles), jnp.sin(angles)


def apply_rope(values, cos_tab, sin_tab):
    pair_view = values.reshape(values.shape[:-1] + (HEAD_DIM // 2, 2))
    even_part = pair_view[..., 0]
    odd_part = pair_view[..., 1]
    cos_b = cos_tab[:, None, :]
    sin_b = sin_tab[:, None, :]
    rotated = jnp.stack([even_part * cos_b - odd_part * sin_b, even_part * sin_b + odd_part * cos_b], axis=-1)
    return rotated.reshape(values.shape)


def attention_core(q_raw, k_raw, v_heads, q_norm, k_norm, cos_tab, sin_tab):
    seq_len, n_heads = q_raw.shape[0], q_raw.shape[1]
    n_kv = k_raw.shape[1]
    q_rot = apply_rope(layer_norm32(q_raw, q_norm), cos_tab, sin_tab).astype(jnp.bfloat16)
    k_rot = apply_rope(layer_norm32(k_raw, k_norm), cos_tab, sin_tab).astype(jnp.bfloat16)
    q_grp = q_rot.reshape(seq_len, n_kv, n_heads // n_kv, HEAD_DIM)
    scores = jnp.einsum('qkgd,skd->kgqs', q_grp.astype(jnp.float32), k_rot.astype(jnp.float32)) * HEAD_DIM ** -0.5
    causal = jnp.arange(seq_len)[:, None] >= jnp.arange(seq_len)[None, :]
    attn_prob = jax.nn.softmax(jnp.where(causal, scores, -1e30), axis=-1).astype(jnp.bfloat16)
    context = jnp.einsum('kgqs,skd->qkgd', attn_prob.astype(jnp.float32), v_heads.astype(jnp.float32))
    return context.astype(jnp.bfloat16).reshape(seq_len, n_heads * HEAD_DIM)


def swiglu(gate_proj, up_proj):
    return jax.nn.silu(gate_proj) * up_proj


def layer_forward(stream, params, cos_tab, sin_tab):
    ln_gamma, w_q, w_k, w_v, w_o, w_gate, w_up, w_down, q_norm, k_norm = params
    lead_shape = stream.shape[:-1]
    n_heads = w_q.shape[1] // HEAD_DIM
    n_kv = w_k.shape[1] // HEAD_DIM
    x_f32 = stream.astype(jnp.float32)
    normed = layer_norm32(x_f32, ln_gamma).astype(jnp.bfloat16)
    q_raw = jnp.dot(normed, w_q, preferred_element_type=jnp.float32).reshape(lead_shape + (n_heads, HEAD_DIM))
    k_raw = jnp.dot(normed, w_k, preferred_element_type=jnp.float32).reshape(lead_shape + (n_kv, HEAD_DIM))
    v_heads = jnp.dot(normed, w_v, preferred_element_type=jnp.float32).astype(jnp.bfloat16).reshape(lead_shape + (n_kv, HEAD_DIM))
    attn_out = attention_core(q_raw, k_raw, v_heads, q_norm.reshape(n_heads, HEAD_DIM), k_norm.reshape(n_kv, HEAD_DIM), cos_tab, sin_tab)
    gate_proj = jnp.dot(normed, w_gate, preferred_element_type=jnp.float32)
    up_proj = jnp.dot(normed, w_up, preferred_element_type=jnp.float32)
    hidden = swiglu(gate_proj, up_proj).astype(jnp.bfloat16)
    layer_sum = x_f32 + jnp.dot(attn_out, w_o, preferred_element_type=jnp.float32) + jnp.dot(hidden, w_down, preferred_element_type=jnp.float32)
    saved_acts = (stream, normed, q_raw, k_raw, v_heads, attn_out, gate_proj, up_proj, hidden)
    return layer_sum.astype(jnp.bfloat16), saved_acts


def layer_backward(grad_y, saved_acts, params, cos_tab, sin_tab):
    ln_gamma, w_q, w_k, w_v, w_o, w_gate, w_up, w_down, q_norm, k_norm = params
    stream, normed, q_raw, k_raw, v_heads, attn_out, gate_proj, up_proj, hidden = saved_acts
    seq_len = stream.shape[0]
    n_heads = q_raw.shape[1]
    n_kv = k_raw.shape[1]
    g_w_down = jnp.dot(hidden.T, grad_y, preferred_element_type=jnp.float32)
    g_w_o = jnp.dot(attn_out.T, grad_y, preferred_element_type=jnp.float32)
    d_hidden = jnp.dot(grad_y, w_down.T, preferred_element_type=jnp.float32)
    swiglu_vjp = jax.vjp(swiglu, gate_proj, up_proj)[1]
    d_gate, d_up = swiglu_vjp(d_hidden)
    d_gate = d_gate.astype(jnp.bfloat16)
    d_up = d_up.astype(jnp.bfloat16)
    g_w_gate = jnp.dot(normed.T, d_gate, preferred_element_type=jnp.float32)
    g_w_up = jnp.dot(normed.T, d_up, preferred_element_type=jnp.float32)
    d_attn = jnp.dot(grad_y, w_o.T, preferred_element_type=jnp.float32).astype(jnp.bfloat16)
    core_fn = functools.partial(attention_core, cos_tab=cos_tab, sin_tab=sin_tab)
    core_vjp = jax.vjp(core_fn, q_raw, k_raw, v_heads, q_norm.reshape(n_heads, HEAD_DIM), k_norm.reshape(n_kv, HEAD_DIM))[1]
    d_qraw, d_kraw, d_vheads, g_q_norm, g_k_norm = core_vjp(d_attn)
    d_q = d_qraw.astype(jnp.bfloat16).reshape(seq_len, n_heads * HEAD_DIM)
    d_k = d_kraw.astype(jnp.bfloat16).reshape(seq_len, n_kv * HEAD_DIM)
    d_v = d_vheads.reshape(seq_len, n_kv * HEAD_DIM)
    g_w_q = jnp.dot(normed.T, d_q, preferred_element_type=jnp.float32)
    g_w_k = jnp.dot(normed.T, d_k, preferred_element_type=jnp.float32)
    g_w_v = jnp.dot(normed.T, d_v, preferred_element_type=jnp.float32)
    d_normed = (jnp.dot(d_gate, w_gate.T, preferred_element_type=jnp.float32)
                + jnp.dot(d_up, w_up.T, preferred_element_type=jnp.float32)
                + jnp.dot(d_q, w_q.T, preferred_element_type=jnp.float32)
                + jnp.dot(d_k, w_k.T, preferred_element_type=jnp.float32)
                + jnp.dot(d_v, w_v.T, preferred_element_type=jnp.float32))
    norm_vjp = jax.vjp(layer_norm32, stream.astype(jnp.float32), ln_gamma)[1]
    d_stream, g_ln_gamma = norm_vjp(d_normed)
    grad_x = (grad_y.astype(jnp.float32) + d_stream).astype(jnp.bfloat16)
    grads = (g_ln_gamma, g_w_q, g_w_k, g_w_v, g_w_o, g_w_gate, g_w_up, g_w_down, g_q_norm.reshape(-1), g_k_norm.reshape(-1))
    return grad_x, grads


def reference(x_in, positions, grad_out, ln_gamma_1, w_q_1, w_k_1, w_v_1, w_o_1, w_gate_1, w_up_1, w_down_1, q_norm_1, k_norm_1, ln_gamma_2, w_q_2, w_k_2, w_v_2, w_o_2, w_gate_2, w_up_2, w_down_2, q_norm_2, k_norm_2):
    cos_tab, sin_tab = rope_tables(positions)
    layers = ((ln_gamma_1, w_q_1, w_k_1, w_v_1, w_o_1, w_gate_1, w_up_1, w_down_1, q_norm_1, k_norm_1),
              (ln_gamma_2, w_q_2, w_k_2, w_v_2, w_o_2, w_gate_2, w_up_2, w_down_2, q_norm_2, k_norm_2))
    zero_grads = tuple(tuple(jnp.zeros(param_piece.shape, jnp.float32) for param_piece in layer_params) for layer_params in layers)

    def one_sequence(grad_sums, seq_pair):
        stream, seq_grad = seq_pair
        saved_list = []
        for layer_params in layers:
            stream, saved_acts = layer_forward(stream, layer_params, cos_tab, sin_tab)
            saved_list.append(saved_acts)
        new_sums = list(grad_sums)
        for layer_index in (1, 0):
            seq_grad, grads = layer_backward(seq_grad, saved_list[layer_index], layers[layer_index], cos_tab, sin_tab)
            new_sums[layer_index] = tuple(acc_grad + part_grad for acc_grad, part_grad in zip(grad_sums[layer_index], grads))
        return tuple(new_sums), (stream, seq_grad)

    grad_sums, outputs = lax.scan(one_sequence, zero_grads, (x_in, grad_out))
    return (outputs[0], outputs[1]) + grad_sums[0] + grad_sums[1]
```

```python
import jax
import jax.numpy as jnp
from jax import lax
from jax.experimental import pallas as pl
from jax.experimental.pallas import tpu as pltpu
from jax.sharding import Mesh, PartitionSpec as P


HEAD_DIM = 128
EPSILON = 1e-5
ROPE_THETA = 7.5e7
AX = ('z', 'y', 'x', 'c')
CHIP_AXES = ('z', 'y', 'x')
BIT = {'z': 4, 'y': 2, 'x': 1}
SWAP = [(0, 1), (1, 0)]
F32 = jnp.float32
BF16 = jnp.bfloat16


def layer_norm32(values, weight):
    row_mean = jnp.mean(values, axis=-1, keepdims=True)
    centered = values - row_mean
    variance = jnp.mean(centered * centered, axis=-1, keepdims=True)
    return centered * lax.rsqrt(variance + EPSILON) * weight


def rope_tables(positions):
    inv_freq = ROPE_THETA ** (-jnp.arange(0, HEAD_DIM, 2, dtype=F32) / HEAD_DIM)
    angles = positions.astype(F32)[:, None] * inv_freq[None, :]
    cos_tab, sin_tab = jnp.cos(angles), jnp.sin(angles)
    cos_full = jnp.repeat(cos_tab, 2, axis=1)
    sin_full = jnp.stack([-sin_tab, sin_tab], axis=-1).reshape(cos_full.shape)
    return cos_full, sin_full


def swap_pairs(values):
    lane = lax.broadcasted_iota(jnp.int32, values.shape, 1)
    return jnp.where((lane & 1) == 0, pltpu.roll(values, HEAD_DIM - 1, 1), pltpu.roll(values, 1, 1))


def head_stats(values):
    centered = values - jnp.mean(values, axis=-1, keepdims=True)
    scale = lax.rsqrt(jnp.mean(centered * centered, axis=-1, keepdims=True) + EPSILON)
    return centered * scale, scale


def rotate(values, cos_full, sin_full):
    return (values * cos_full + swap_pairs(values) * sin_full).astype(BF16)


def contract(a, b, dim_a, dim_b):
    return lax.dot_general(a, b, (((dim_a,), (dim_b,)), ((), ())), preferred_element_type=F32)


def softmax_rows(q_rot, k_rot):
    scores = contract(q_rot, k_rot, 1, 1) * HEAD_DIM ** -0.5
    row = lax.broadcasted_iota(jnp.int32, scores.shape, 0)
    col = lax.broadcasted_iota(jnp.int32, scores.shape, 1)
    scores = jnp.where(row >= col, scores, -1e30)
    expo = jnp.exp(scores - jnp.max(scores, axis=-1, keepdims=True))
    return expo / jnp.sum(expo, axis=-1, keepdims=True)


def attn_fwd_kernel(q_ref, k_ref, v_ref, qn_ref, kn_ref, cos_ref, sin_ref, o_ref):
    cos_full, sin_full = cos_ref[...], sin_ref[...]
    k_hat, _ = head_stats(k_ref[...])
    k_rot = rotate(k_hat * kn_ref[0], cos_full, sin_full)
    v_head = v_ref[...].astype(BF16)
    for g in range(q_ref.shape[1] // HEAD_DIM):
        cols = slice(g * HEAD_DIM, (g + 1) * HEAD_DIM)
        q_hat, _ = head_stats(q_ref[:, cols])
        q_rot = rotate(q_hat * qn_ref[0, g:g + 1], cos_full, sin_full)
        prob = softmax_rows(q_rot, k_rot).astype(BF16)
        o_ref[:, cols] = contract(prob, v_head, 1, 0).astype(BF16)


def norm_bwd(d_rot, hat, scale, weight, cos_full, sin_full):
    d_val = d_rot.astype(BF16).astype(F32)
    d_out = d_val * cos_full + swap_pairs(d_val * sin_full)
    g_weight = jnp.sum(d_out * hat, axis=0, keepdims=True)
    d_hat = d_out * weight
    mean_d = jnp.mean(d_hat, axis=-1, keepdims=True)
    mean_dh = jnp.mean(d_hat * hat, axis=-1, keepdims=True)
    return (scale * (d_hat - mean_d - hat * mean_dh)).astype(BF16), g_weight


def attn_bwd_kernel(q_ref, k_ref, v_ref, do_ref, qn_ref, kn_ref, cos_ref, sin_ref, dqkv_ref, gq_ref, gk_ref):
    head = pl.program_id(0)
    n_kv = pl.num_programs(0)
    group = q_ref.shape[1] // HEAD_DIM
    cos_full, sin_full = cos_ref[...], sin_ref[...]
    k_hat, k_scale = head_stats(k_ref[...])
    k_rot = rotate(k_hat * kn_ref[0], cos_full, sin_full)
    v_head = v_ref[...].astype(BF16)
    dv = jnp.zeros(v_head.shape, F32)
    dk = jnp.zeros(v_head.shape, F32)
    for g in range(group):
        cols = slice(g * HEAD_DIM, (g + 1) * HEAD_DIM)
        q_hat, q_scale = head_stats(q_ref[:, cols])
        q_rot = rotate(q_hat * qn_ref[0, g:g + 1], cos_full, sin_full)
        prob = softmax_rows(q_rot, k_rot)
        d_out = do_ref[:, cols]
        dv = dv + contract(prob.astype(BF16), d_out, 0, 0)
        d_prob = contract(d_out, v_head, 1, 1).astype(BF16).astype(F32)
        d_score = prob * (d_prob - jnp.sum(d_prob * prob, axis=-1, keepdims=True))
        d_score = (d_score * HEAD_DIM ** -0.5).astype(BF16)
        dk = dk + contract(d_score, q_rot, 0, 0)
        dq, g_q = norm_bwd(contract(d_score, k_rot, 1, 0), q_hat, q_scale, qn_ref[0, g:g + 1], cos_full, sin_full)
        dqkv_ref[:, pl.ds(pl.multiple_of((head * group + g) * HEAD_DIM, HEAD_DIM), HEAD_DIM)] = dq
        gq_ref[0, g:g + 1] = g_q
    dk_raw, g_k = norm_bwd(dk, k_hat, k_scale, kn_ref[0], cos_full, sin_full)
    base = n_kv * group + head
    dqkv_ref[:, pl.ds(pl.multiple_of(base * HEAD_DIM, HEAD_DIM), HEAD_DIM)] = dk_raw
    dqkv_ref[:, pl.ds(pl.multiple_of((base + n_kv) * HEAD_DIM, HEAD_DIM), HEAD_DIM)] = dv.astype(BF16)
    gk_ref[0] = g_k


def qkv_specs(seq_len, n_kv, group):
    q_spec = pl.BlockSpec((seq_len, group * HEAD_DIM), lambda j: (0, j))
    k_spec = pl.BlockSpec((seq_len, HEAD_DIM), lambda j: (0, n_kv * group + j))
    v_spec = pl.BlockSpec((seq_len, HEAD_DIM), lambda j: (0, n_kv * group + n_kv + j))
    qn_spec = pl.BlockSpec((1, group, HEAD_DIM), lambda j: (j, 0, 0))
    kn_spec = pl.BlockSpec((1, 1, HEAD_DIM), lambda j: (j, 0, 0))
    tab_spec = pl.BlockSpec((seq_len, HEAD_DIM), lambda j: (0, 0))
    return q_spec, k_spec, v_spec, qn_spec, kn_spec, tab_spec


def attention_fwd(qkv, q_norm, k_norm, cos_full, sin_full):
    seq_len, n_kv, group = qkv.shape[0], k_norm.shape[0], q_norm.shape[1]
    q_spec, k_spec, v_spec, qn_spec, kn_spec, tab_spec = qkv_specs(seq_len, n_kv, group)
    return pl.pallas_call(
        attn_fwd_kernel,
        grid=(n_kv,),
        in_specs=[q_spec, k_spec, v_spec, qn_spec, kn_spec, tab_spec, tab_spec],
        out_specs=q_spec,
        out_shape=jax.ShapeDtypeStruct((seq_len, n_kv * group * HEAD_DIM), BF16),
        cost_estimate=pl.CostEstimate(flops=1_500_000_000, bytes_accessed=12_000_000, transcendentals=0),
        name='attn_fwd',
    )(qkv, qkv, qkv, q_norm, k_norm, cos_full, sin_full)


def attention_bwd(qkv, d_attn, q_norm, k_norm, cos_full, sin_full):
    seq_len, n_kv, group = qkv.shape[0], k_norm.shape[0], q_norm.shape[1]
    q_spec, k_spec, v_spec, qn_spec, kn_spec, tab_spec = qkv_specs(seq_len, n_kv, group)
    return pl.pallas_call(
        attn_bwd_kernel,
        grid=(n_kv,),
        in_specs=[q_spec, k_spec, v_spec, q_spec, qn_spec, kn_spec, tab_spec, tab_spec],
        out_specs=[pl.BlockSpec(qkv.shape, lambda j: (0, 0)), qn_spec, kn_spec],
        out_shape=[jax.ShapeDtypeStruct(qkv.shape, BF16), jax.ShapeDtypeStruct(q_norm.shape, F32), jax.ShapeDtypeStruct(k_norm.shape, F32)],
        cost_estimate=pl.CostEstimate(flops=4_000_000_000, bytes_accessed=15_000_000, transcendentals=0),
        name='attn_bwd',
    )(qkv, qkv, qkv, d_attn, q_norm, k_norm, cos_full, sin_full)


def swiglu(gate_proj, up_proj):
    return jax.nn.silu(gate_proj) * up_proj


def dot32(a, b):
    return jnp.dot(a, b, preferred_element_type=F32)


def dot_t32(a, b):
    return lax.dot_general(a, b, (((1,), (1,)), ((), ())), preferred_element_type=F32)


def swap_cores(value):
    return lax.ppermute(value, 'c', SWAP)


def pair_rows(act, block_rows, chip_pos, core):
    act_t = act.T
    tokens = act_t.shape[1]

    def pick(which):
        parts = []
        for delta in range(8):
            chip = 0
            for axis in CHIP_AXES:
                chip = chip + BIT[axis] * (chip_pos[axis] ^ (1 if delta & BIT[axis] else 0))
            start = (chip * 2 + which) * block_rows
            parts.append(lax.dynamic_slice(act_t, (start, 0), (block_rows, tokens)))
        return jnp.concatenate(parts, axis=0)

    mine = pick(core)
    theirs = swap_cores(pick(1 - core))
    both = jnp.concatenate([mine, theirs], axis=1)
    return [both[d * block_rows:(d + 1) * block_rows] for d in range(8)]


def pair_tokens(cot):
    pair = lax.optimization_barrier((cot, swap_cores(cot)))
    return jnp.concatenate(pair, axis=0)


def hop(value, axis):
    return lax.ppermute(value, axis, SWAP)


def reduce_group(blocks, cot, dims):
    rows = blocks[0].shape[0]

    def part(b1, b2, b3):
        return blocks[b1 * BIT[dims[0]] + b2 * BIT[dims[1]] + b3 * BIT[dims[2]]]

    send1 = dot32(jnp.concatenate([part(1, 0, 0), part(1, 0, 1), part(1, 1, 0), part(1, 1, 1)], axis=0), cot)
    got1 = hop(send1, dims[0])
    send2 = dot32(jnp.concatenate([part(0, 1, 0), part(0, 1, 1)], axis=0), cot) + got1[2 * rows:]
    got2 = hop(send2, dims[1])
    send3 = dot32(part(0, 0, 1), cot) + got1[rows:2 * rows] + got2[rows:]
    got3 = hop(send3, dims[2])
    return dot32(part(0, 0, 0), cot) + got1[:rows] + got2[:rows] + got3


def scatter_small(values, chip_pos, core):
    value = values.reshape((2, 2, 2, 2) + values.shape[1:])
    for axis, pos in (('c', core), ('x', chip_pos['x']), ('y', chip_pos['y']), ('z', chip_pos['z'])):
        dim = {'z': 0, 'y': 1, 'x': 2, 'c': 3}[axis]
        keep = lax.dynamic_index_in_dim(value, pos, dim, keepdims=False)
        send = lax.dynamic_index_in_dim(value, 1 - pos, dim, keepdims=False)
        value = keep + lax.ppermute(send, axis, SWAP)
    return value


RING = {
    'o': ('z', 'x', 'y'),
    'down': ('x', 'y', 'z'),
    'gate': ('y', 'z', 'x'),
    'up': ('z', 'x', 'y'),
    'q': ('x', 'y', 'z'),
    'kv': ('y', 'z', 'x'),
}


def layer_specs():
    vector_spec = P(AX)
    matrix_spec = P(AX, None)
    return (vector_spec,) + (matrix_spec,) * 7 + (vector_spec, vector_spec)


def solution(mesh):
    cube = Mesh(mesh.devices.reshape(2, 2, 2, 2), AX)
    act_spec = P(AX, None, None)
    param_spec = layer_specs()
    in_specs = (act_spec, P(), act_spec) + param_spec + param_spec
    out_specs = (act_spec, act_spec) + param_spec + param_spec

    def inner(x_in, positions, grad_out, *shards):
        layer_shards = [shards[:10], shards[10:]]
        chip_pos = {axis: lax.axis_index(axis) for axis in CHIP_AXES}
        core = lax.axis_index('c')

        def gather(piece):
            return lax.all_gather(piece, AX, axis=0, tiled=True)

        cos_full, sin_full = rope_tables(positions)

        weights = []
        for _, w_q, w_k, w_v, w_o, w_gate, w_up, w_down, _, _ in layer_shards:
            w_in = gather(jnp.concatenate([w_q, w_k, w_v, w_gate, w_up], axis=1))
            qkv_width = w_q.shape[1] + w_k.shape[1] + w_v.shape[1]
            w_qkv, w_gu = w_in[:, :qkv_width], w_in[:, qkv_width:]
            w_od = gather(jnp.concatenate([w_o, w_down], axis=0))
            rows_o, rows_d = w_o.shape[0], w_down.shape[0]
            w_od = w_od.reshape(16, rows_o + rows_d, -1)
            weights.append((w_qkv, w_gu, w_od[:, :rows_o].reshape(16 * rows_o, -1), w_od[:, rows_o:].reshape(16 * rows_d, -1)))
        vecs = jnp.concatenate([v for s in layer_shards for v in (s[0], s[8], s[9])])
        vec_sizes = [v.shape[0] for s in layer_shards for v in (s[0], s[8], s[9])]
        vecs = lax.all_gather(vecs, AX, axis=0, tiled=False)
        small, offset = [], 0
        for size in vec_sizes:
            small.append(vecs[:, offset:offset + size].reshape(-1))
            offset += size

        stream = x_in[0]
        saved = []
        for layer in range(2):
            w_qkv, w_gu, w_o_full, w_down_full = weights[layer]
            ln_gamma = small[3 * layer]
            n_kv = small[3 * layer + 2].shape[0] // HEAD_DIM
            q_norm = small[3 * layer + 1].reshape(n_kv, -1, HEAD_DIM)
            k_norm = small[3 * layer + 2].reshape(n_kv, 1, HEAD_DIM)
            q_width, kv_width = q_norm.size, k_norm.size
            x_f32 = stream.astype(F32)
            normed32, norm_vjp = jax.vjp(layer_norm32, x_f32, ln_gamma)
            normed = normed32.astype(BF16)
            qkv = dot32(normed, w_qkv)
            attn_out = attention_fwd(qkv, q_norm, k_norm, cos_full, sin_full)
            gate_up = dot32(normed, w_gu)
            ffn = gate_up.shape[1] // 2
            hidden32, swiglu_vjp = jax.vjp(swiglu, gate_up[:, :ffn], gate_up[:, ffn:])
            hidden = hidden32.astype(BF16)
            layer_sum = x_f32 + dot32(attn_out, w_o_full) + dot32(hidden, w_down_full)
            stream = layer_sum.astype(BF16)
            saved.append((norm_vjp, normed, qkv, q_norm, k_norm, attn_out, swiglu_vjp, hidden, q_width, kv_width))

        grad = grad_out[0]
        out_grads = [None, None]
        small_grads = [None, None]
        for layer in (1, 0):
            norm_vjp, normed, qkv, q_norm, k_norm, attn_out, swiglu_vjp, hidden, q_width, kv_width = saved[layer]
            w_qkv, w_gu, w_o_full, w_down_full = weights[layer]
            ffn = hidden.shape[1]
            grad2 = pair_tokens(grad)
            attn_rows = pair_rows(attn_out, attn_out.shape[1] // 16, chip_pos, core)
            g_o = reduce_group(attn_rows, grad2, RING['o'])
            hidden_rows = pair_rows(hidden, ffn // 16, chip_pos, core)
            g_down = reduce_group(hidden_rows, grad2, RING['down'])
            d_hidden = dot_t32(grad, w_down_full)
            d_gate, d_up = swiglu_vjp(d_hidden)
            d_gu = jnp.concatenate([d_gate.astype(BF16), d_up.astype(BF16)], axis=1)
            normed_rows = pair_rows(normed, normed.shape[1] // 16, chip_pos, core)
            d_gu2 = pair_tokens(d_gu)
            g_gate = reduce_group(normed_rows, d_gu2[:, :ffn], RING['gate'])
            g_up = reduce_group(normed_rows, d_gu2[:, ffn:], RING['up'])
            d_attn = dot_t32(grad, w_o_full).astype(BF16)
            d_qkv, g_q_norm, g_k_norm = attention_bwd(qkv, d_attn, q_norm, k_norm, cos_full, sin_full)
            d_qkv2 = pair_tokens(d_qkv)
            g_q = reduce_group(normed_rows, d_qkv2[:, :q_width], RING['q'])
            g_kv = reduce_group(normed_rows, d_qkv2[:, q_width:], RING['kv'])
            d_normed = dot_t32(d_gu, w_gu) + dot_t32(d_qkv, w_qkv)
            d_stream, g_ln = norm_vjp(d_normed)
            grad = (grad.astype(F32) + d_stream).astype(BF16)
            small_grads[layer] = jnp.concatenate([g_ln.reshape(16, -1), g_q_norm.reshape(16, -1), g_k_norm.reshape(16, -1)], axis=1)
            out_grads[layer] = (g_q, g_kv[:, :kv_width], g_kv[:, kv_width:], g_o, g_gate, g_up, g_down)
        small_sum = scatter_small(jnp.concatenate(small_grads, axis=1), chip_pos, core)
        pieces, offset = [], 0
        for size in vec_sizes:
            pieces.append(small_sum[offset:offset + size])
            offset += size
        outs = []
        for layer in range(2):
            outs += [pieces[3 * layer], *out_grads[layer], pieces[3 * layer + 1], pieces[3 * layer + 2]]
        return (stream[None], grad[None], *outs)

    return jax.shard_map(inner, mesh=cube, in_specs=in_specs, out_specs=out_specs, check_vma=False)
```

```python
import jax
import jax.numpy as jnp
from jax import lax
from jax.experimental import pallas as pl
from jax.experimental.pallas import tpu as pltpu
from jax.sharding import Mesh, PartitionSpec as P


HEAD_DIM = 128
EPSILON = 1e-5
ROPE_THETA = 7.5e7
AX = ('z', 'y', 'x', 'c')
CHIP_AXES = ('z', 'y', 'x')
BIT = {'z': 4, 'y': 2, 'x': 1}
SWAP = [(0, 1), (1, 0)]
F32 = jnp.float32
BF16 = jnp.bfloat16


def layer_norm32(values, weight):
    row_mean = jnp.mean(values, axis=-1, keepdims=True)
    centered = values - row_mean
    variance = jnp.mean(centered * centered, axis=-1, keepdims=True)
    return centered * lax.rsqrt(variance + EPSILON) * weight


def rope_tables(positions):
    inv_freq = ROPE_THETA ** (-jnp.arange(0, HEAD_DIM, 2, dtype=F32) / HEAD_DIM)
    angles = positions.astype(F32)[:, None] * inv_freq[None, :]
    cos_tab, sin_tab = jnp.cos(angles), jnp.sin(angles)
    cos_full = jnp.repeat(cos_tab, 2, axis=1)
    sin_full = jnp.stack([-sin_tab, sin_tab], axis=-1).reshape(cos_full.shape)
    return cos_full, sin_full


def swap_pairs(values):
    lane = lax.broadcasted_iota(jnp.int32, values.shape, 1)
    return jnp.where((lane & 1) == 0, pltpu.roll(values, HEAD_DIM - 1, 1), pltpu.roll(values, 1, 1))


def head_stats(values):
    centered = values - jnp.mean(values, axis=-1, keepdims=True)
    scale = lax.rsqrt(jnp.mean(centered * centered, axis=-1, keepdims=True) + EPSILON)
    return centered * scale, scale


def rotate(values, cos_full, sin_full):
    return (values * cos_full + swap_pairs(values) * sin_full).astype(BF16)


def contract(a, b, dim_a, dim_b):
    return lax.dot_general(a, b, (((dim_a,), (dim_b,)), ((), ())), preferred_element_type=F32)


def softmax_rows(q_rot, k_rot):
    scores = contract(q_rot, k_rot, 1, 1) * HEAD_DIM ** -0.5
    row = lax.broadcasted_iota(jnp.int32, scores.shape, 0)
    col = lax.broadcasted_iota(jnp.int32, scores.shape, 1)
    scores = jnp.where(row >= col, scores, -1e30)
    expo = jnp.exp(scores - jnp.max(scores, axis=-1, keepdims=True))
    return expo / jnp.sum(expo, axis=-1, keepdims=True)


def attn_fwd_kernel(q_ref, k_ref, v_ref, qn_ref, kn_ref, cos_ref, sin_ref, o_ref):
    cos_full, sin_full = cos_ref[...], sin_ref[...]
    k_hat, _ = head_stats(k_ref[...])
    k_rot = rotate(k_hat * kn_ref[0], cos_full, sin_full)
    v_head = v_ref[...].astype(BF16)
    for g in range(q_ref.shape[1] // HEAD_DIM):
        cols = slice(g * HEAD_DIM, (g + 1) * HEAD_DIM)
        q_hat, _ = head_stats(q_ref[:, cols])
        q_rot = rotate(q_hat * qn_ref[0, g:g + 1], cos_full, sin_full)
        prob = softmax_rows(q_rot, k_rot).astype(BF16)
        o_ref[:, cols] = contract(prob, v_head, 1, 0).astype(BF16)


def norm_bwd(d_rot, hat, scale, weight, cos_full, sin_full):
    d_val = d_rot.astype(BF16).astype(F32)
    d_out = d_val * cos_full + swap_pairs(d_val * sin_full)
    g_weight = jnp.sum(d_out * hat, axis=0, keepdims=True)
    d_hat = d_out * weight
    mean_d = jnp.mean(d_hat, axis=-1, keepdims=True)
    mean_dh = jnp.mean(d_hat * hat, axis=-1, keepdims=True)
    return (scale * (d_hat - mean_d - hat * mean_dh)).astype(BF16), g_weight


def attn_bwd_kernel(q_ref, k_ref, v_ref, do_ref, qn_ref, kn_ref, cos_ref, sin_ref, dqkv_ref, gq_ref, gk_ref):
    head = pl.program_id(0)
    n_kv = pl.num_programs(0)
    group = q_ref.shape[1] // HEAD_DIM
    cos_full, sin_full = cos_ref[...], sin_ref[...]
    k_hat, k_scale = head_stats(k_ref[...])
    k_rot = rotate(k_hat * kn_ref[0], cos_full, sin_full)
    v_head = v_ref[...].astype(BF16)
    dv = jnp.zeros(v_head.shape, F32)
    dk = jnp.zeros(v_head.shape, F32)
    for g in range(group):
        cols = slice(g * HEAD_DIM, (g + 1) * HEAD_DIM)
        q_hat, q_scale = head_stats(q_ref[:, cols])
        q_rot = rotate(q_hat * qn_ref[0, g:g + 1], cos_full, sin_full)
        prob = softmax_rows(q_rot, k_rot)
        d_out = do_ref[:, cols]
        dv = dv + contract(prob.astype(BF16), d_out, 0, 0)
        d_prob = contract(d_out, v_head, 1, 1).astype(BF16).astype(F32)
        d_score = prob * (d_prob - jnp.sum(d_prob * prob, axis=-1, keepdims=True))
        d_score = (d_score * HEAD_DIM ** -0.5).astype(BF16)
        dk = dk + contract(d_score, q_rot, 0, 0)
        dq, g_q = norm_bwd(contract(d_score, k_rot, 1, 0), q_hat, q_scale, qn_ref[0, g:g + 1], cos_full, sin_full)
        dqkv_ref[:, pl.ds(pl.multiple_of((head * group + g) * HEAD_DIM, HEAD_DIM), HEAD_DIM)] = dq
        gq_ref[0, g:g + 1] = g_q
    dk_raw, g_k = norm_bwd(dk, k_hat, k_scale, kn_ref[0], cos_full, sin_full)
    base = n_kv * group + head
    dqkv_ref[:, pl.ds(pl.multiple_of(base * HEAD_DIM, HEAD_DIM), HEAD_DIM)] = dk_raw
    dqkv_ref[:, pl.ds(pl.multiple_of((base + n_kv) * HEAD_DIM, HEAD_DIM), HEAD_DIM)] = dv.astype(BF16)
    gk_ref[0] = g_k


def qkv_specs(seq_len, n_kv, group):
    q_spec = pl.BlockSpec((seq_len, group * HEAD_DIM), lambda j: (0, j))
    k_spec = pl.BlockSpec((seq_len, HEAD_DIM), lambda j: (0, n_kv * group + j))
    v_spec = pl.BlockSpec((seq_len, HEAD_DIM), lambda j: (0, n_kv * group + n_kv + j))
    qn_spec = pl.BlockSpec((1, group, HEAD_DIM), lambda j: (j, 0, 0))
    kn_spec = pl.BlockSpec((1, 1, HEAD_DIM), lambda j: (j, 0, 0))
    tab_spec = pl.BlockSpec((seq_len, HEAD_DIM), lambda j: (0, 0))
    return q_spec, k_spec, v_spec, qn_spec, kn_spec, tab_spec


def attention_fwd(qkv, q_norm, k_norm, cos_full, sin_full):
    seq_len, n_kv, group = qkv.shape[0], k_norm.shape[0], q_norm.shape[1]
    q_spec, k_spec, v_spec, qn_spec, kn_spec, tab_spec = qkv_specs(seq_len, n_kv, group)
    return pl.pallas_call(
        attn_fwd_kernel,
        grid=(n_kv,),
        in_specs=[q_spec, k_spec, v_spec, qn_spec, kn_spec, tab_spec, tab_spec],
        out_specs=q_spec,
        out_shape=jax.ShapeDtypeStruct((seq_len, n_kv * group * HEAD_DIM), BF16),
        cost_estimate=pl.CostEstimate(flops=1_500_000_000, bytes_accessed=12_000_000, transcendentals=0),
        name='attn_fwd',
    )(qkv, qkv, qkv, q_norm, k_norm, cos_full, sin_full)


def attention_bwd(qkv, d_attn, q_norm, k_norm, cos_full, sin_full):
    seq_len, n_kv, group = qkv.shape[0], k_norm.shape[0], q_norm.shape[1]
    q_spec, k_spec, v_spec, qn_spec, kn_spec, tab_spec = qkv_specs(seq_len, n_kv, group)
    return pl.pallas_call(
        attn_bwd_kernel,
        grid=(n_kv,),
        in_specs=[q_spec, k_spec, v_spec, q_spec, qn_spec, kn_spec, tab_spec, tab_spec],
        out_specs=[pl.BlockSpec(qkv.shape, lambda j: (0, 0)), qn_spec, kn_spec],
        out_shape=[jax.ShapeDtypeStruct(qkv.shape, BF16), jax.ShapeDtypeStruct(q_norm.shape, F32), jax.ShapeDtypeStruct(k_norm.shape, F32)],
        cost_estimate=pl.CostEstimate(flops=4_000_000_000, bytes_accessed=15_000_000, transcendentals=0),
        name='attn_bwd',
    )(qkv, qkv, qkv, d_attn, q_norm, k_norm, cos_full, sin_full)


def swiglu(gate_proj, up_proj):
    return jax.nn.silu(gate_proj) * up_proj


def dot32(a, b):
    return jnp.dot(a, b, preferred_element_type=F32)


def dot_t32(a, b):
    return lax.dot_general(a, b, (((1,), (1,)), ((), ())), preferred_element_type=F32)


def swap_cores(value):
    return lax.ppermute(value, 'c', SWAP)


def pair_rows_kernel(index_ref, act_ref, mine_ref, theirs_ref, flip_ref):
    rows = mine_ref.shape[0]
    core = index_ref[8]
    flip_ref[...] = act_ref[...].T
    mine_ref[...] = flip_ref[pl.ds(pl.multiple_of(core * rows, rows), rows), :]
    theirs_ref[...] = flip_ref[pl.ds(pl.multiple_of((1 - core) * rows, rows), rows), :]


def pair_rows(act, dims, chip_pos, core):
    tokens = act.shape[0]
    rows = act.shape[1] // 16
    deltas = [sum(BIT[dims[i]] * ((d >> (2 - i)) & 1) for i in range(3)) for d in range(8)]
    chip = sum(BIT[axis] * chip_pos[axis] for axis in CHIP_AXES)
    index = jnp.stack([chip ^ delta for delta in deltas] + [core]).astype(jnp.int32)
    out_spec = pl.BlockSpec((rows, tokens), lambda d, idx: (d, 0))
    mine, theirs = pl.pallas_call(
        pair_rows_kernel,
        grid_spec=pltpu.PrefetchScalarGridSpec(
            num_scalar_prefetch=1,
            grid=(8,),
            in_specs=[pl.BlockSpec((tokens, 2 * rows), lambda d, idx: (0, idx[d]))],
            out_specs=[out_spec, out_spec],
            scratch_shapes=[pltpu.VMEM((2 * rows, tokens), BF16)],
        ),
        out_shape=[jax.ShapeDtypeStruct((8 * rows, tokens), BF16)] * 2,
        cost_estimate=pl.CostEstimate(flops=300_000_000, bytes_accessed=4 * act.size, transcendentals=0),
        name='pair_rows',
    )(index, act)
    both = jnp.concatenate([mine, swap_cores(theirs)], axis=1)
    return {delta: both[d * rows:(d + 1) * rows] for d, delta in enumerate(deltas)}


def pair_tokens(cot):
    pair = lax.optimization_barrier((cot, swap_cores(cot)))
    return jnp.concatenate(pair, axis=0)


def hop(value, axis):
    return lax.ppermute(value, axis, SWAP)


def reduce_group(blocks, cot, tag, sends):
    rows, dims = blocks[0].shape[0], RING[tag]

    def part(b1, b2, b3):
        return blocks[b1 * BIT[dims[0]] + b2 * BIT[dims[1]] + b3 * BIT[dims[2]]]

    half = jnp.concatenate([part(1, 0, 0), part(1, 0, 1), part(1, 1, 0), part(1, 1, 1)], axis=0)
    quarter = jnp.concatenate([part(0, 1, 0), part(0, 1, 1)], axis=0)
    send1 = dot32(half, cot)
    sends[tag] = send1
    got1 = hop(send1, dims[0])
    send2 = dot32(quarter, cot) + got1[2 * rows:]
    got2 = hop(send2, dims[1])
    send3 = dot32(part(0, 0, 1), cot) + got1[rows:2 * rows] + got2[rows:]
    got3 = hop(send3, dims[2])
    return dot32(part(0, 0, 0), cot) + got1[:rows] + got2[:rows] + got3


def scatter_small(values, chip_pos, core):
    value = values.reshape(8, 2, -1)
    keep = lax.dynamic_index_in_dim(value, core, 1, keepdims=False)
    value = keep + hop(lax.dynamic_index_in_dim(value, 1 - core, 1, keepdims=False), 'c')
    chip = sum(BIT[axis] * chip_pos[axis] for axis in CHIP_AXES)
    total = lax.dynamic_index_in_dim(value, chip, 0, keepdims=False)
    sends = [lax.dynamic_index_in_dim(value, chip ^ delta, 0, keepdims=False) for delta in range(1, 8)]
    gots = [lax.ppermute(send, CHIP_AXES, [(i, i ^ delta) for i in range(8)]) for delta, send in enumerate(sends, 1)]
    return sum(gots, total)


RING = {
    'down_0': ('x', 'y', 'z'),
    'down_1': ('x', 'y', 'z'),
    'gate_0': ('y', 'z', 'x'),
    'gate_1': ('y', 'z', 'x'),
    'kv_0': ('y', 'z', 'x'),
    'kv_1': ('y', 'z', 'x'),
    'o_0': ('z', 'x', 'y'),
    'o_1': ('z', 'x', 'y'),
    'q_0': ('x', 'y', 'z'),
    'q_1': ('x', 'y', 'z'),
    'up_0': ('z', 'x', 'y'),
    'up_1': ('z', 'x', 'y'),
}


def layer_specs():
    vector_spec = P(AX)
    matrix_spec = P(AX, None)
    return (vector_spec,) + (matrix_spec,) * 7 + (vector_spec, vector_spec)


def solution(mesh):
    cube = Mesh(mesh.devices.reshape(2, 2, 2, 2), AX)
    act_spec = P(AX, None, None)
    param_spec = layer_specs()
    in_specs = (act_spec, P(), act_spec) + param_spec + param_spec
    out_specs = (act_spec, act_spec) + param_spec + param_spec

    def inner(x_in, positions, grad_out, *shards):
        layer_shards = [shards[:10], shards[10:]]
        chip_pos = {axis: lax.axis_index(axis) for axis in CHIP_AXES}
        core = lax.axis_index('c')

        def gather(piece):
            return lax.all_gather(piece, AX, axis=0, tiled=True)

        cos_full, sin_full = rope_tables(positions)

        weights = []
        for layer, (_, w_q, w_k, w_v, w_o, w_gate, w_up, w_down, _, _) in enumerate(layer_shards):
            in_cols = jnp.concatenate([w_q, w_k, w_v, w_gate, w_up], axis=1)
            qkv_width = w_q.shape[1] + w_k.shape[1] + w_v.shape[1]
            in_width = in_cols.shape[1]
            rows_in, rows_o, rows_d = w_q.shape[0], w_o.shape[0], w_down.shape[0]
            if layer == 0:
                stacked = [m[i * rows_in:(i + 1) * rows_in] for m in (w_o, w_down) for i in range(m.shape[0] // rows_in)]
                w_all = gather(jnp.concatenate([in_cols] + stacked, axis=1))
                w_in = w_all[:, :in_width]
                width = w_o.shape[1]
                w_od = jnp.concatenate([w_all[:, in_width + i * width:in_width + (i + 1) * width].reshape(16, rows_in, width) for i in range(len(stacked))], axis=1)
            else:
                w_in = gather(in_cols)
                w_od = gather(jnp.concatenate([w_o, w_down], axis=0)).reshape(16, rows_o + rows_d, -1)
            w_qkv, w_gu = w_in[:, :qkv_width], w_in[:, qkv_width:]
            weights.append((w_qkv, w_gu, w_od))
        vecs = jnp.concatenate([v for s in layer_shards for v in (s[0], s[8], s[9])])
        vec_sizes = [v.shape[0] for s in layer_shards for v in (s[0], s[8], s[9])]
        vecs = lax.all_gather(vecs, AX, axis=0, tiled=False)
        small, offset = [], 0
        for size in vec_sizes:
            small.append(vecs[:, offset:offset + size].reshape(-1))
            offset += size

        def split_od(w_od):
            return w_od[:, :rows_o].reshape(16 * rows_o, -1), w_od[:, rows_o:].reshape(16 * rows_d, -1)

        def layer_out(x_f32, attn_out, hidden, w_o_full, w_down_full):
            layer_sum = x_f32 + dot32(attn_out, w_o_full) + dot32(hidden, w_down_full)
            return layer_sum.astype(BF16)

        stream = x_in[0]
        saved = []
        for layer in range(2):
            w_qkv, w_gu, w_od = weights[layer]
            ln_gamma = small[3 * layer]
            n_kv = small[3 * layer + 2].shape[0] // HEAD_DIM
            q_norm = small[3 * layer + 1].reshape(n_kv, -1, HEAD_DIM)
            k_norm = small[3 * layer + 2].reshape(n_kv, 1, HEAD_DIM)
            q_width, kv_width = q_norm.size, k_norm.size
            x_f32 = stream.astype(F32)
            normed32, norm_vjp = jax.vjp(layer_norm32, x_f32, ln_gamma)
            normed = normed32.astype(BF16)
            qkv = dot32(normed, w_qkv)
            attn_out = attention_fwd(qkv, q_norm, k_norm, cos_full, sin_full)
            gate_up = dot32(normed, w_gu)
            ffn = gate_up.shape[1] // 2
            hidden32, swiglu_vjp = jax.vjp(swiglu, gate_up[:, :ffn], gate_up[:, ffn:])
            hidden = hidden32.astype(BF16)
            if layer == 0:
                od_pair = split_od(w_od)
                stream = layer_out(x_f32, attn_out, hidden, *od_pair)
            saved.append((x_f32, norm_vjp, normed, qkv, q_norm, k_norm, attn_out, swiglu_vjp, hidden, q_width, kv_width))

        grad = grad_out[0]
        out_grads = [None, None]
        sends = {}
        small_grads = [None, None]
        for layer in (1, 0):
            x_f32, norm_vjp, normed, qkv, q_norm, k_norm, attn_out, swiglu_vjp, hidden, q_width, kv_width = saved[layer]
            w_qkv, w_gu, w_od = weights[layer]
            ffn = hidden.shape[1]
            grad2 = pair_tokens(grad)
            attn_rows = pair_rows(attn_out, RING['o_' + str(layer)], chip_pos, core)
            g_o = reduce_group(attn_rows, grad2, 'o_' + str(layer), sends)
            hidden_rows = pair_rows(hidden, RING['down_' + str(layer)], chip_pos, core)
            g_down = reduce_group(hidden_rows, grad2, 'down_' + str(layer), sends)
            if layer == 1:
                w_od, _ = lax.optimization_barrier((w_od, sends['down_1']))
                w_o_full, w_down_full = split_od(w_od)
                stream = layer_out(x_f32, attn_out, hidden, w_o_full, w_down_full)
            else:
                w_o_full, w_down_full = od_pair
            d_hidden = dot_t32(grad, w_down_full)
            d_gate, d_up = swiglu_vjp(d_hidden)
            d_gu = jnp.concatenate([d_gate.astype(BF16), d_up.astype(BF16)], axis=1)
            normed_rows = pair_rows(normed, CHIP_AXES, chip_pos, core)
            d_gu2 = pair_tokens(d_gu)
            g_gate = reduce_group(normed_rows, d_gu2[:, :ffn], 'gate_' + str(layer), sends)
            g_up = reduce_group(normed_rows, d_gu2[:, ffn:], 'up_' + str(layer), sends)
            d_attn = dot_t32(grad, w_o_full).astype(BF16)
            d_qkv, g_q_norm, g_k_norm = attention_bwd(qkv, d_attn, q_norm, k_norm, cos_full, sin_full)
            d_qkv2 = pair_tokens(d_qkv)
            g_q = reduce_group(normed_rows, d_qkv2[:, :q_width], 'q_' + str(layer), sends)
            g_kv = reduce_group(normed_rows, d_qkv2[:, q_width:], 'kv_' + str(layer), sends)
            d_normed = dot_t32(d_gu, w_gu) + dot_t32(d_qkv, w_qkv)
            d_stream, g_ln = norm_vjp(d_normed)
            grad = (grad.astype(F32) + d_stream).astype(BF16)
            small_grads[layer] = jnp.concatenate([g_ln.reshape(16, -1), g_q_norm.reshape(16, -1), g_k_norm.reshape(16, -1)], axis=1)
            out_grads[layer] = (g_q, g_kv[:, :kv_width], g_kv[:, kv_width:], g_o, g_gate, g_up, g_down)
        small_sum = scatter_small(jnp.concatenate(small_grads, axis=1), chip_pos, core)
        pieces, offset = [], 0
        for size in vec_sizes:
            pieces.append(small_sum[offset:offset + size])
            offset += size
        outs = []
        for layer in range(2):
            outs += [pieces[3 * layer], *out_grads[layer], pieces[3 * layer + 1], pieces[3 * layer + 2]]
        return (stream[None], grad[None], *outs)

    return jax.shard_map(inner, mesh=cube, in_specs=in_specs, out_specs=out_specs, check_vma=False)
```
